32 devices in a mesh: gx: 2 (over x), gy: 4 (over y, core), gz: 4 (over z).
Axes of the slice: x: 2, y: 2, z: 4, core: 2. Of those that a mesh axis runs over, the one named last changes fastest.
Arguments:
- tokens: bfloat16 [1024, 4608], P('gx', 'gy'), may hold values from -6 to 6
- base_up_weight: bfloat16 [4608, 18432], P('gy', ('gz', 'gx')), may hold values from -0.09375 to 0.09375
- adapter_down_weight: bfloat16 [64, 16, 4608], P(None, None, 'gy'), may hold values from -0.09375 to 0.09375
- adapter_up_weight: bfloat16 [64, 16, 18432], P('gx', None, 'gz'), may hold values from -1.5 to 1.5
- block_adapter_index: int32 [8], P('gx'), may hold values from 0 to 63
- request_rows: int32 [8], P('gx'), may hold values from 1 to 128
Outputs:
- projected: bfloat16 [1024, 18432], P(('gx', 'gy'), 'gz')
The draws below stay inside these ranges and needn't reach their ends.
Inputs may be any that keep to these rules, and one draw needn't show every extreme that they name: `request_rows`: live rows of each block.
All inputs are finite; a program needn't handle non-finite values.
Results may differ from the reference program's by a relative error of at most 0.0047.
Values may be sent and summed in bfloat16 or wider, within the bound.
A program may use at most 128 MiB of HBM per device.

```python
import jax
import jax.numpy as jnp
from jax import lax

MODEL_WIDTH = 4608
HIDDEN_UNITS = 18432
ADAPTER_RANK = 16
ADAPTER_COUNT = 64
BLOCK = 128
BLOCKS = 8
ROWS = 1024


def touch_ends(array, rng, low, largest):
    place = [jax.random.randint(jax.random.fold_in(rng, axis), (), 0, length) for axis, length in enumerate(array.shape)]
    main_axis = array.shape.index(max(array.shape))
    beside = place[:main_axis] + [(place[main_axis] + 1) % array.shape[main_axis]] + place[main_axis + 1:]
    return array.at[tuple(place)].set(low).at[tuple(beside)].set(largest)


def block_scale(own_key, shape, pieces, least, high):
    factor_of = 1.0
    for axis_at, parts in pieces:
        steps = jax.random.uniform(jax.random.fold_in(jax.random.fold_in(own_key, 6), axis_at), (parts,), jnp.float32, least / len(pieces), high / len(pieces))
        factor_of = factor_of * jnp.repeat(jnp.exp(steps), shape[axis_at] // parts).reshape((-1,) + (1,) * (len(shape) - 1 - axis_at))
    return factor_of


def gaussian(key, dims, scale, most, shards=(), kind=jnp.bfloat16):
    values = scale * jax.random.normal(key, dims, jnp.float32)
    if shards:
        values = values * block_scale(key, dims, shards, -0.22, 0.18)
    return jnp.clip(values, -most, most).astype(kind)


def setup_inputs(seed: int = 0) -> dict:
    streams_of = jax.random.split(jax.random.key(seed), 7)
    return {
        "tokens": gaussian(streams_of[0], (ROWS, MODEL_WIDTH), 1.0, 6.0, ((0, 2), (1, 4))),
        "base_up_weight": gaussian(streams_of[1], (MODEL_WIDTH, HIDDEN_UNITS), MODEL_WIDTH ** -0.5, 0.09375, ((0, 4), (1, 8))),
        "adapter_down_weight": gaussian(streams_of[2], (ADAPTER_COUNT, ADAPTER_RANK, MODEL_WIDTH), MODEL_WIDTH ** -0.5, 0.09375, ((2, 4),)),
        "adapter_up_weight": gaussian(streams_of[3], (ADAPTER_COUNT, ADAPTER_RANK, HIDDEN_UNITS), ADAPTER_RANK ** -0.5, 1.5, ((0, 2), (2, 4))),
        "block_adapter_index": touch_ends(jax.random.randint(streams_of[4], (BLOCKS,), 0, ADAPTER_COUNT), jax.random.fold_in(streams_of[4], 1), 0, ADAPTER_COUNT - 1).astype(jnp.int32),
        "request_rows": touch_ends(jax.random.randint(streams_of[5], (BLOCKS,), 1, BLOCK + 1), jax.random.fold_in(streams_of[5], 1), 1, BLOCK).astype(jnp.int32),
    }


def reference(tokens, base_up_weight, adapter_down_weight, adapter_up_weight, block_adapter_index, request_rows):
    blocks = block_adapter_index.shape[0]
    tok_blocks = tokens.reshape(blocks, BLOCK, MODEL_WIDTH)

    def one_block(items):
        block_tokens, adapter_index, live_count = items
        down_factor = lax.dynamic_index_in_dim(adapter_down_weight, adapter_index, 0, keepdims=False)
        up_factor = lax.dynamic_index_in_dim(adapter_up_weight, adapter_index, 0, keepdims=False)
        shrink = jnp.dot(block_tokens, down_factor.T, preferred_element_type=jnp.float32)
        shrink_low = shrink.astype(jnp.bfloat16)
        expand = jnp.dot(shrink_low, up_factor, preferred_element_type=jnp.float32)
        base = jnp.dot(block_tokens, base_up_weight, preferred_element_type=jnp.float32)
        live_mask = jnp.arange(BLOCK, dtype=jnp.int32) < live_count
        return jnp.where(live_mask[:, None], base + 2.0 * expand, 0.0).astype(jnp.bfloat16)

    result = lax.map(one_block, (tok_blocks, block_adapter_index, request_rows))
    return result.reshape(blocks * BLOCK, HIDDEN_UNITS)
```

```python
import functools

import jax
import jax.numpy as jnp
from jax import lax
from jax.experimental import pallas as pl
from jax.experimental.pallas import tpu as pltpu
from jax.sharding import PartitionSpec as P

F32 = jnp.float32
BF16 = jnp.bfloat16
PIECES = 2


def general_body(
    tokens,
    base_up_weight,
    adapter_down_weight,
    adapter_up_weight,
    block_adapter_index,
    request_rows,
):
    rows, shard_width = tokens.shape
    groups = lax.axis_size("gy")
    blocks = block_adapter_index.shape[0]
    block = rows // blocks
    own_blocks = blocks // groups
    own_rows = own_blocks * block
    first = lax.axis_index("gy") * own_blocks
    count, rank_values, _ = adapter_down_weight.shape
    catalog = jnp.arange(count, dtype=jnp.int32)
    selected_adapters = (block_adapter_index[:, None] == catalog[None, :]).astype(BF16)
    chosen_down = jnp.dot(
        selected_adapters,
        adapter_down_weight.reshape(count, rank_values * shard_width),
        preferred_element_type=F32,
    )
    chosen_down = chosen_down.astype(BF16).reshape(blocks, rank_values, shard_width)
    tok_blocks = tokens.reshape(blocks, block, shard_width)
    shrink_part = jnp.einsum("bmd,brd->bmr", tok_blocks, chosen_down, preferred_element_type=F32)
    shrink_own = lax.psum_scatter(shrink_part, "gy", scatter_dimension=0, tiled=True)
    shrink_low = shrink_own.astype(BF16)
    adapter_factors = lax.all_gather(adapter_up_weight, "gx", axis=0, tiled=True)
    out_width = adapter_factors.shape[2]
    own_picks = lax.dynamic_slice_in_dim(selected_adapters, first, own_blocks, 0)
    chosen_up = jnp.dot(
        own_picks,
        adapter_factors.reshape(count, rank_values * out_width),
        preferred_element_type=F32,
    )
    chosen_up = chosen_up.astype(BF16).reshape(own_blocks, rank_values, out_width)
    expand = jnp.einsum("bmr,brf->bmf", shrink_low, chosen_up, preferred_element_type=F32)
    expand = expand.reshape(own_rows, out_width)
    partial_value = jnp.dot(
        tokens,
        lax.all_gather(base_up_weight, "gx", axis=1, tiled=True),
        preferred_element_type=F32,
    )
    extra = 2.0 * expand
    total = lax.psum_scatter(partial_value, "gy", scatter_dimension=0, tiled=True) + extra
    own_live = lax.dynamic_slice_in_dim(request_rows, first, own_blocks, 0)
    live_mask = (jnp.arange(block, dtype=jnp.int32)[None, :] < own_live[:, None]).reshape(
        own_rows, 1
    )
    return jnp.where(live_mask, total, 0.0).astype(BF16)


def kernel(
    chunks,
    index_ref,
    live_ref,
    tok_hbm,
    w_hbm,
    down_hbm,
    up_hbm,
    out_ref,
    tok,
    far_tok,
    w,
    down,
    up,
    pick,
    pick_in,
    up_own,
    up_send,
    up_in,
    shrink_own,
    shrink_send,
    shrink_in,
    a_send,
    a_in,
    keep,
    b_send,
    b_in,
    c_send,
    c_in,
    local_sem,
    a_sem,
    b_sem,
    c_sem,
    x_sem,
    z_sem,
    pick_sem,
    up_sem,
    shrink_sem,
):
    gx = lax.axis_index("gx")
    gy = lax.axis_index("gy")
    gz = lax.axis_index("gz")
    core = lax.rem(gy, 2)
    yy = lax.div(gy, 2)
    y_far = 1 - yy
    zp = lax.rem(gz, 2)
    x_peer = {"gx": 1 - gx}
    core_peer = {"gy": gy + 1 - 2 * core}
    y_peer = {"gy": lax.rem(gy + 2, 4)}
    diagonal = {"gy": 3 - gy}
    z_peer = {"gz": gz + 1 - 2 * zp}
    block = out_ref.shape[0]
    cols = w.shape[1]
    wide = cols // chunks
    ranks = down.shape[1]
    held = up.shape[0]
    piece = block // PIECES

    def remote(src, dst, sems, n, device):
        return pltpu.make_async_remote_copy(
            src_ref=src,
            dst_ref=dst,
            send_sem=sems.at[0, n],
            recv_sem=sems.at[1, n],
            device_id=device,
            device_id_type=pl.DeviceIdType.MESH,
        )

    tok_load = pltpu.make_async_copy(tok_hbm, tok, local_sem.at[0])
    tok_load.start()
    w_loads = []
    for n in range(chunks):
        span = pl.ds(n * wide, wide)
        load = pltpu.make_async_copy(w_hbm.at[:, span], w.at[:, span], local_sem.at[3 + n])
        load.start()
        w_loads.append(load)
    down_load = pltpu.make_async_copy(down_hbm, down, local_sem.at[1])
    down_load.start()
    up_load = pltpu.make_async_copy(up_hbm, up, local_sem.at[2])
    up_load.start()

    barrier = pltpu.get_barrier_semaphore()
    for device in (x_peer, core_peer, y_peer, diagonal, z_peer):
        pl.semaphore_signal(
            barrier, inc=1, device_id=device, device_id_type=pl.DeviceIdType.MESH
        )

    wanted = index_ref[gy]
    rank_at = lax.broadcasted_iota(jnp.int32, (ranks, held), 0)
    slot_at = lax.broadcasted_iota(jnp.int32, (ranks, held), 1)
    for half in range(2):
        hit = slot_at + half * held == wanted * ranks + rank_at
        pick[half] = jnp.where(hit, 1.0, 0.0).astype(BF16)

    pl.semaphore_wait(barrier, 5)
    tok_load.wait()

    x_copies, z_copies = [], []
    for u, y_at in enumerate((y_far, yy)):
        for q in range(PIECES):
            at = pl.multiple_of((2 * y_at + zp) * block + q * piece, piece)
            n = u * PIECES + q
            span = pl.ds(at, piece)
            copy = remote(tok.at[span, :], far_tok.at[span, :], x_sem, n, x_peer)
            copy.start()
            x_copies.append(copy)
            z_copies.append(remote(far_tok.at[span, :], far_tok.at[span, :], z_sem, n, z_peer))
    pick_copy = remote(pick.at[1 - gx], pick_in, pick_sem, 0, x_peer)
    pick_copy.start()

    def row(c):
        return pl.ds(pl.multiple_of(c * block, block), block)

    a_copies, b_copies, c_copies = {}, {}, {}

    def multiply(tokens_ref, g, u, y_at, n):
        s = (g * 2 + u) * chunks + n
        lhs = tokens_ref[pl.ds(pl.multiple_of(y_at * 2 * block, 2 * block), 2 * block), :]
        part = jnp.dot(lhs, w[:, n * wide : (n + 1) * wide], preferred_element_type=F32)
        low, high = part[:block], part[block:]
        mine = core == 0
        a_send[s] = jnp.where(mine, high, low)
        keep[s] = jnp.where(mine, low, high)
        copy = remote(a_send.at[s], a_in.at[s], a_sem, s, core_peer)
        copy.start()
        a_copies[s] = copy

    def pair_up(g, u, n):
        s = (g * 2 + u) * chunks + n
        a_copies[s].wait_recv()
        both = keep[s] + a_in[s]
        if u == 0:
            k = g * chunks + n
            b_send[k] = both.astype(BF16)
            copy = remote(b_send.at[k], b_in.at[k], b_sem, k, y_peer)
            copy.start()
            b_copies[k] = copy
        else:
            keep[s] = both

    def relay(n):
        x_copies[n].wait_recv()
        z_copies[n].start()

    waiting = None
    for u, y_at in enumerate((y_far, yy)):
        for n in range(chunks):
            if u == 0:
                w_loads[n].wait()
            multiply(tok, 0, u, y_at, n)
            if waiting is not None:
                pair_up(*waiting)
            waiting = (0, u, n)
    pair_up(*waiting)

    relay(0)
    down_load.wait()
    shrink_copies = []
    for d, (device, at) in enumerate(
        (
            (core_peer, core_peer["gy"]),
            (y_peer, y_peer["gy"]),
            (diagonal, diagonal["gy"]),
            (None, gy),
        )
    ):
        value = lax.dot_general(
            down[index_ref[at]],
            tok[row(at), :],
            (((1,), (1,)), ((), ())),
            preferred_element_type=F32,
        )
        if device is None:
            shrink_own[...] = value
        else:
            shrink_send[d] = value
            copy = remote(shrink_send.at[d], shrink_in.at[d], shrink_sem, d, device)
            copy.start()
            shrink_copies.append(copy)
    relay(1)
    pick_copy.wait_recv()
    up_load.wait()
    up_width = up.shape[1]
    for n in range(2 * chunks):
        span = slice(n * wide, (n + 1) * wide)
        up_own[:, span] = jnp.dot(
            pick[gx], up[:, span], preferred_element_type=F32
        ).astype(BF16)
        up_send[:, span] = jnp.dot(
            pick_in[...], up[:, span], preferred_element_type=F32
        ).astype(BF16)
    up_copy = remote(up_send, up_in, up_sem, 0, x_peer)
    up_copy.start()

    relay(2)
    for n in range(PIECES):
        z_copies[n].wait_recv()
    waiting = None
    for n in range(chunks):
        multiply(far_tok, 1, 0, y_far, n)
        if waiting is not None:
            pair_up(*waiting)
        waiting = (1, 0, n)
    pair_up(*waiting)
    for n in range(3, 2 * PIECES):
        relay(n)
    for n in range(PIECES, 2 * PIECES):
        z_copies[n].wait_recv()
    waiting = None
    for n in range(chunks):
        multiply(far_tok, 1, 1, yy, n)
        if waiting is not None:
            pair_up(*waiting)
        waiting = (1, 1, n)
    pair_up(*waiting)

    for copy in shrink_copies:
        copy.wait_recv()
    shrink = (shrink_own[...] + shrink_in[0]) + (shrink_in[1] + shrink_in[2])
    shrink_low = shrink.astype(BF16)
    up_copy.wait_recv()
    live = lax.broadcasted_iota(jnp.int32, (block, 1), 0) < live_ref[gy]

    def finish(side, n, base):
        span = pl.ds(pl.multiple_of(side * cols + n * wide, 128), wide)
        factor = up_own[:, span] + up_in[:, span]
        expand = lax.dot_general(
            shrink_low, factor, (((0,), (0,)), ((), ())), preferred_element_type=F32
        )
        out_ref[:, span] = jnp.where(live, base + 2.0 * expand, 0.0).astype(BF16)

    for n in range(chunks):
        b_copies[n].wait_recv()
        finish(gx, n, keep[chunks + n] + b_in[n].astype(F32))
    for n in range(chunks):
        k = chunks + n
        b_copies[k].wait_recv()
        c_send[n] = (keep[3 * chunks + n] + b_in[k].astype(F32)).astype(BF16)
        copy = remote(c_send.at[n], c_in.at[n], c_sem, n, x_peer)
        copy.start()
        c_copies[n] = copy
    for n in range(chunks):
        c_copies[n].wait_recv()
        finish(1 - gx, n, c_in[n].astype(F32))

    for copy in (
        x_copies
        + z_copies
        + [pick_copy, up_copy]
        + shrink_copies
        + list(a_copies.values())
        + list(b_copies.values())
        + list(c_copies.values())
    ):
        copy.wait_send()


def fused_body(
    tokens,
    base_up_weight,
    adapter_down_weight,
    adapter_up_weight,
    block_adapter_index,
    request_rows,
):
    rows, depth = tokens.shape
    cols = base_up_weight.shape[1]
    block = rows // block_adapter_index.shape[0]
    count, ranks, _ = adapter_down_weight.shape
    held_count, _, out_width = adapter_up_weight.shape
    held = held_count * ranks
    chunks = cols // max(n for n in range(256, 769, 256) if cols % n == 0)
    wide = cols // chunks
    steps = 4 * chunks
    anywhere = pl.BlockSpec(memory_space=pl.ANY)
    smem = pl.BlockSpec(memory_space=pltpu.SMEM)

    def dma(n):
        return pltpu.SemaphoreType.DMA((2, n))

    return pl.pallas_call(
        functools.partial(kernel, chunks),
        out_shape=jax.ShapeDtypeStruct((block, out_width), BF16),
        in_specs=[smem, smem, anywhere, anywhere, anywhere, anywhere],
        out_specs=pl.BlockSpec(memory_space=pltpu.VMEM),
        scratch_shapes=[
            pltpu.VMEM((rows, depth), BF16),
            pltpu.VMEM((rows, depth), BF16),
            pltpu.VMEM((depth, cols), BF16),
            pltpu.VMEM((count, ranks, depth), BF16),
            pltpu.VMEM((held, out_width), BF16),
            pltpu.VMEM((2, ranks, held), BF16),
            pltpu.VMEM((ranks, held), BF16),
            pltpu.VMEM((ranks, out_width), BF16),
            pltpu.VMEM((ranks, out_width), BF16),
            pltpu.VMEM((ranks, out_width), BF16),
            pltpu.VMEM((ranks, block), F32),
            pltpu.VMEM((3, ranks, block), F32),
            pltpu.VMEM((3, ranks, block), F32),
            pltpu.VMEM((steps, block, wide), F32),
            pltpu.VMEM((steps, block, wide), F32),
            pltpu.VMEM((steps, block, wide), F32),
            pltpu.VMEM((2 * chunks, block, wide), BF16),
            pltpu.VMEM((2 * chunks, block, wide), BF16),
            pltpu.VMEM((chunks, block, wide), BF16),
            pltpu.VMEM((chunks, block, wide), BF16),
            pltpu.SemaphoreType.DMA((3 + chunks,)),
            dma(steps),
            dma(2 * chunks),
            dma(chunks),
            dma(2 * PIECES),
            dma(2 * PIECES),
            dma(1),
            dma(1),
            dma(3),
        ],
        compiler_params=pltpu.CompilerParams(
            collective_id=0, has_side_effects=True, vmem_limit_bytes=60 * 1024 * 1024
        ),
    )(
        block_adapter_index,
        request_rows,
        tokens,
        base_up_weight,
        adapter_down_weight,
        adapter_up_weight.reshape(held, out_width),
    )


def solution(mesh):
    in_specs = (
        P("gx", "gy"),
        P("gy", ("gz", "gx")),
        P(None, None, "gy"),
        P("gx", None, "gz"),
        P("gx"),
        P("gx"),
    )
    out_specs = P(("gx", "gy"), "gz")
    sizes = mesh.shape

    def body(*arrays):
        blocks = arrays[4].shape[0]
        paired = sizes["gx"] == 2 and sizes["gy"] == 4 and sizes["gz"] % 2 == 0
        if paired and blocks == sizes["gy"]:
            return fused_body(*arrays)
        return general_body(*arrays)

    return jax.shard_map(body, mesh=mesh, in_specs=in_specs, out_specs=out_specs, check_vma=False)
```

```python
import functools

import jax
import jax.numpy as jnp
from jax import lax
from jax.experimental import pallas as pl
from jax.experimental.pallas import tpu as pltpu
from jax.sharding import PartitionSpec as P

F32 = jnp.float32
BF16 = jnp.bfloat16
PIECES = 1


def general_body(
    tokens,
    base_up_weight,
    adapter_down_weight,
    adapter_up_weight,
    block_adapter_index,
    request_rows,
):
    rows, shard_width = tokens.shape
    groups = lax.axis_size("gy")
    blocks = block_adapter_index.shape[0]
    block = rows // blocks
    own_blocks = blocks // groups
    own_rows = own_blocks * block
    first = lax.axis_index("gy") * own_blocks
    count, rank_values, _ = adapter_down_weight.shape
    catalog = jnp.arange(count, dtype=jnp.int32)
    selected_adapters = (block_adapter_index[:, None] == catalog[None, :]).astype(BF16)
    chosen_down = jnp.dot(
        selected_adapters,
        adapter_down_weight.reshape(count, rank_values * shard_width),
        preferred_element_type=F32,
    )
    chosen_down = chosen_down.astype(BF16).reshape(blocks, rank_values, shard_width)
    tok_blocks = tokens.reshape(blocks, block, shard_width)
    shrink_part = jnp.einsum("bmd,brd->bmr", tok_blocks, chosen_down, preferred_element_type=F32)
    shrink_own = lax.psum_scatter(shrink_part, "gy", scatter_dimension=0, tiled=True)
    shrink_low = shrink_own.astype(BF16)
    adapter_factors = lax.all_gather(adapter_up_weight, "gx", axis=0, tiled=True)
    out_width = adapter_factors.shape[2]
    own_picks = lax.dynamic_slice_in_dim(selected_adapters, first, own_blocks, 0)
    chosen_up = jnp.dot(
        own_picks,
        adapter_factors.reshape(count, rank_values * out_width),
        preferred_element_type=F32,
    )
    chosen_up = chosen_up.astype(BF16).reshape(own_blocks, rank_values, out_width)
    expand = jnp.einsum("bmr,brf->bmf", shrink_low, chosen_up, preferred_element_type=F32)
    expand = expand.reshape(own_rows, out_width)
    partial_value = jnp.dot(
        tokens,
        lax.all_gather(base_up_weight, "gx", axis=1, tiled=True),
        preferred_element_type=F32,
    )
    extra = 2.0 * expand
    total = lax.psum_scatter(partial_value, "gy", scatter_dimension=0, tiled=True) + extra
    own_live = lax.dynamic_slice_in_dim(request_rows, first, own_blocks, 0)
    live_mask = (jnp.arange(block, dtype=jnp.int32)[None, :] < own_live[:, None]).reshape(
        own_rows, 1
    )
    return jnp.where(live_mask, total, 0.0).astype(BF16)


def kernel(
    chunks,
    index_ref,
    live_ref,
    tok_hbm,
    w_hbm,
    down_hbm,
    up_hbm,
    out_ref,
    tok,
    far_tok,
    w,
    down,
    up,
    pick,
    pick_in,
    up_own,
    up_send,
    up_in,
    shrink_own,
    shrink_send,
    shrink_in,
    a_send,
    a_in,
    keep,
    b_send,
    b_in,
    c_send,
    c_in,
    local_sem,
    a_sem,
    b_sem,
    c_sem,
    x_sem,
    z_sem,
    pick_sem,
    up_sem,
    shrink_sem,
):
    gx = lax.axis_index("gx")
    gy = lax.axis_index("gy")
    gz = lax.axis_index("gz")
    core = lax.rem(gy, 2)
    yy = lax.div(gy, 2)
    y_far = 1 - yy
    zp = lax.rem(gz, 2)
    x_peer = {"gx": 1 - gx}
    core_peer = {"gy": gy + 1 - 2 * core}
    y_peer = {"gy": lax.rem(gy + 2, 4)}
    diagonal = {"gy": 3 - gy}
    z_peer = {"gz": gz + 1 - 2 * zp}
    block = out_ref.shape[0]
    cols = w.shape[1]
    wide = cols // chunks
    ranks = down.shape[1]
    held = up.shape[0]
    piece = block // PIECES

    def remote(src, dst, sems, n, device):
        return pltpu.make_async_remote_copy(
            src_ref=src,
            dst_ref=dst,
            send_sem=sems.at[0, n],
            recv_sem=sems.at[1, n],
            device_id=device,
            device_id_type=pl.DeviceIdType.MESH,
        )

    tok_load = pltpu.make_async_copy(tok_hbm, tok, local_sem.at[0])
    tok_load.start()
    w_loads = []
    for n in range(chunks):
        span = pl.ds(n * wide, wide)
        load = pltpu.make_async_copy(w_hbm.at[:, span], w.at[:, span], local_sem.at[3 + n])
        load.start()
        w_loads.append(load)
    down_load = pltpu.make_async_copy(down_hbm, down, local_sem.at[1])
    down_load.start()
    up_load = pltpu.make_async_copy(up_hbm, up, local_sem.at[2])
    up_load.start()

    barrier = pltpu.get_barrier_semaphore()
    for device in (x_peer, core_peer, y_peer, diagonal, z_peer):
        pl.semaphore_signal(
            barrier, inc=1, device_id=device, device_id_type=pl.DeviceIdType.MESH
        )

    wanted = index_ref[gy]
    rank_at = lax.broadcasted_iota(jnp.int32, (ranks, held), 0)
    slot_at = lax.broadcasted_iota(jnp.int32, (ranks, held), 1)
    for half in range(2):
        hit = slot_at + half * held == wanted * ranks + rank_at
        pick[half] = jnp.where(hit, 1.0, 0.0).astype(BF16)

    pl.semaphore_wait(barrier, 5)
    tok_load.wait()

    x_copies, z_copies = [], []
    for u, y_at in enumerate((y_far, yy)):
        for q in range(PIECES):
            at = pl.multiple_of((2 * y_at + zp) * block + q * piece, piece)
            n = u * PIECES + q
            span = pl.ds(at, piece)
            copy = remote(tok.at[span, :], far_tok.at[span, :], x_sem, n, x_peer)
            copy.start()
            x_copies.append(copy)
            z_copies.append(remote(far_tok.at[span, :], far_tok.at[span, :], z_sem, n, z_peer))
    pick_copy = remote(pick.at[1 - gx], pick_in, pick_sem, 0, x_peer)
    pick_copy.start()

    def row(c):
        return pl.ds(pl.multiple_of(c * block, block), block)

    a_copies, b_copies, c_copies = {}, {}, {}

    def multiply(tokens_ref, g, u, y_at, n):
        s = (g * 2 + u) * chunks + n
        lhs = tokens_ref[pl.ds(pl.multiple_of(y_at * 2 * block, 2 * block), 2 * block), :]
        part = jnp.dot(lhs, w[:, n * wide : (n + 1) * wide], preferred_element_type=F32)
        low, high = part[:block], part[block:]
        mine = core == 0
        a_send[s] = jnp.where(mine, high, low)
        keep[s] = jnp.where(mine, low, high)
        copy = remote(a_send.at[s], a_in.at[s], a_sem, s, core_peer)
        copy.start()
        a_copies[s] = copy

    def pair_up(g, u, n):
        s = (g * 2 + u) * chunks + n
        a_copies[s].wait_recv()
        both = keep[s] + a_in[s]
        if u == 0:
            k = g * chunks + n
            b_send[k] = both.astype(BF16)
            copy = remote(b_send.at[k], b_in.at[k], b_sem, k, y_peer)
            copy.start()
            b_copies[k] = copy
        else:
            keep[s] = both

    def relay(n):
        x_copies[n].wait_recv()
        z_copies[n].start()

    waiting = None
    for u, y_at in enumerate((y_far, yy)):
        for n in range(chunks):
            if u == 0:
                w_loads[n].wait()
            multiply(tok, 0, u, y_at, n)
            if waiting is not None:
                pair_up(*waiting)
            waiting = (0, u, n)
    pair_up(*waiting)

    relay(0)
    down_load.wait()
    shrink_copies = []
    for d, (device, at) in enumerate(
        (
            (core_peer, core_peer["gy"]),
            (y_peer, y_peer["gy"]),
            (diagonal, diagonal["gy"]),
            (None, gy),
        )
    ):
        value = lax.dot_general(
            down[index_ref[at]],
            tok[row(at), :],
            (((1,), (1,)), ((), ())),
            preferred_element_type=F32,
        )
        if device is None:
            shrink_own[...] = value
        else:
            shrink_send[d] = value
            copy = remote(shrink_send.at[d], shrink_in.at[d], shrink_sem, d, device)
            copy.start()
            shrink_copies.append(copy)
    pick_copy.wait_recv()
    up_load.wait()
    up_width = up.shape[1]
    for n in range(2 * chunks):
        span = slice(n * wide, (n + 1) * wide)
        up_own[:, span] = jnp.dot(
            pick[gx], up[:, span], preferred_element_type=F32
        ).astype(BF16)
        up_send[:, span] = jnp.dot(
            pick_in[...], up[:, span], preferred_element_type=F32
        ).astype(BF16)
    up_copy = remote(up_send, up_in, up_sem, 0, x_peer)
    up_copy.start()

    relay(1)
    for n in range(PIECES):
        z_copies[n].wait_recv()
    waiting = None
    for n in range(chunks):
        multiply(far_tok, 1, 0, y_far, n)
        if waiting is not None:
            pair_up(*waiting)
        waiting = (1, 0, n)
    pair_up(*waiting)
    for n in range(2, 2 * PIECES):
        relay(n)
    for n in range(PIECES, 2 * PIECES):
        z_copies[n].wait_recv()
    waiting = None
    for n in range(chunks):
        multiply(far_tok, 1, 1, yy, n)
        if waiting is not None:
            pair_up(*waiting)
        waiting = (1, 1, n)
    pair_up(*waiting)

    for copy in shrink_copies:
        copy.wait_recv()
    shrink = (shrink_own[...] + shrink_in[0]) + (shrink_in[1] + shrink_in[2])
    shrink_low = shrink.astype(BF16)
    up_copy.wait_recv()
    live = lax.broadcasted_iota(jnp.int32, (block, 1), 0) < live_ref[gy]

    def finish(side, n, base):
        span = pl.ds(pl.multiple_of(side * cols + n * wide, 128), wide)
        factor = up_own[:, span] + up_in[:, span]
        expand = lax.dot_general(
            shrink_low, factor, (((0,), (0,)), ((), ())), preferred_element_type=F32
        )
        out_ref[:, span] = jnp.where(live, base + 2.0 * expand, 0.0).astype(BF16)

    for n in range(chunks):
        b_copies[n].wait_recv()
        finish(gx, n, keep[chunks + n] + b_in[n].astype(F32))
    for n in range(chunks):
        k = chunks + n
        b_copies[k].wait_recv()
        c_send[n] = (keep[3 * chunks + n] + b_in[k].astype(F32)).astype(BF16)
        copy = remote(c_send.at[n], c_in.at[n], c_sem, n, x_peer)
        copy.start()
        c_copies[n] = copy
    for n in range(chunks):
        c_copies[n].wait_recv()
        finish(1 - gx, n, c_in[n].astype(F32))

    for copy in (
        x_copies
        + z_copies
        + [pick_copy, up_copy]
        + shrink_copies
        + list(a_copies.values())
        + list(b_copies.values())
        + list(c_copies.values())
    ):
        copy.wait_send()


def fused_body(
    tokens,
    base_up_weight,
    adapter_down_weight,
    adapter_up_weight,
    block_adapter_index,
    request_rows,
):
    rows, depth = tokens.shape
    cols = base_up_weight.shape[1]
    block = rows // block_adapter_index.shape[0]
    count, ranks, _ = adapter_down_weight.shape
    held_count, _, out_width = adapter_up_weight.shape
    held = held_count * ranks
    chunks = cols // max(n for n in range(128, 1153, 128) if cols % n == 0)
    wide = cols // chunks
    steps = 4 * chunks
    anywhere = pl.BlockSpec(memory_space=pl.ANY)
    smem = pl.BlockSpec(memory_space=pltpu.SMEM)

    def dma(n):
        return pltpu.SemaphoreType.DMA((2, n))

    return pl.pallas_call(
        functools.partial(kernel, chunks),
        out_shape=jax.ShapeDtypeStruct((block, out_width), BF16),
        in_specs=[smem, smem, anywhere, anywhere, anywhere, anywhere],
        out_specs=pl.BlockSpec(memory_space=pltpu.VMEM),
        scratch_shapes=[
            pltpu.VMEM((rows, depth), BF16),
            pltpu.VMEM((rows, depth), BF16),
            pltpu.VMEM((depth, cols), BF16),
            pltpu.VMEM((count, ranks, depth), BF16),
            pltpu.VMEM((held, out_width), BF16),
            pltpu.VMEM((2, ranks, held), BF16),
            pltpu.VMEM((ranks, held), BF16),
            pltpu.VMEM((ranks, out_width), BF16),
            pltpu.VMEM((ranks, out_width), BF16),
            pltpu.VMEM((ranks, out_width), BF16),
            pltpu.VMEM((ranks, block), F32),
            pltpu.VMEM((3, ranks, block), F32),
            pltpu.VMEM((3, ranks, block), F32),
            pltpu.VMEM((steps, block, wide), F32),
            pltpu.VMEM((steps, block, wide), F32),
            pltpu.VMEM((steps, block, wide), F32),
            pltpu.VMEM((2 * chunks, block, wide), BF16),
            pltpu.VMEM((2 * chunks, block, wide), BF16),
            pltpu.VMEM((chunks, block, wide), BF16),
            pltpu.VMEM((chunks, block, wide), BF16),
            pltpu.SemaphoreType.DMA((3 + chunks,)),
            dma(steps),
            dma(2 * chunks),
            dma(chunks),
            dma(2 * PIECES),
            dma(2 * PIECES),
            dma(1),
            dma(1),
            dma(3),
        ],
        compiler_params=pltpu.CompilerParams(
            collective_id=0, has_side_effects=True, vmem_limit_bytes=60 * 1024 * 1024
        ),
    )(
        block_adapter_index,
        request_rows,
        tokens,
        base_up_weight,
        adapter_down_weight,
        adapter_up_weight.reshape(held, out_width),
    )


def solution(mesh):
    in_specs = (
        P("gx", "gy"),
        P("gy", ("gz", "gx")),
        P(None, None, "gy"),
        P("gx", None, "gz"),
        P("gx"),
        P("gx"),
    )
    out_specs = P(("gx", "gy"), "gz")
    sizes = mesh.shape

    def body(*arrays):
        blocks = arrays[4].shape[0]
        paired = sizes["gx"] == 2 and sizes["gy"] == 4 and sizes["gz"] % 2 == 0
        if paired and blocks == sizes["gy"]:
            return fused_body(*arrays)
        return general_body(*arrays)

    return jax.shard_map(body, mesh=mesh, in_specs=in_specs, out_specs=out_specs, check_vma=False)
```
